128 devices in a mesh: row: 8 (over y, core), col: 16 (over z, x).
Axes of the slice: x: 4, y: 4, z: 4, core: 2. Of those that a mesh axis runs over, the one named last changes fastest.
Arguments:
- coefficients: float32 [20480, 1024], P(('row', 'col')), may hold values from -24 to 24, as said below
Outputs:
- orbitals: float32 [20480, 1024], P(('row', 'col'))
The draws below stay inside these ranges and needn't reach their ends.
Inputs may be any that keep to these rules, and one draw needn't show every extreme that they name: Real coefficients of full column rank.
All inputs are finite; a program needn't handle non-finite values.
Results may differ from the reference program's by a relative error of at most 0.00014.
Values sent between devices are 32-bit elements; how exact they have to be, the bound alone decides.
A program may use at most 64 MiB of HBM per device.

```python
import jax
import jax.numpy as jnp
from jax import lax

NB = 1024
PW_DEV = 160
NG = 20480
DEVICES = 128


coupling_rank = 12


coupling_scale = 0.3


spike_factor = 3.0


def draw_coefficients(key, part):
    key_noise, key_sign, key_mix, key_perm = jax.random.split(key, 4)
    noise = jax.random.normal(key_noise, (NG, NB), jnp.float32)
    signs = jnp.where(jax.random.bernoulli(key_sign, 0.5, (NG, coupling_rank)), 1.0, -1.0).astype(jnp.float32)
    mixing = jax.random.normal(key_mix, (coupling_rank, NB), jnp.float32)
    coupled = coupling_scale * jnp.dot(signs, mixing, precision=lax.Precision.HIGHEST, preferred_element_type=jnp.float32)
    paired_block = jax.random.permutation(key_perm, DEVICES).astype(jnp.int32)
    row_block = jnp.arange(NG, dtype=jnp.int32) // PW_DEV
    column_group = jnp.arange(NB, dtype=jnp.int32) % DEVICES
    paired = column_group[None, :] == paired_block[row_block][:, None]
    noise = noise * jnp.where(paired, spike_factor, 1.0).astype(jnp.float32)
    return jnp.clip(noise + coupled, -24.0, 24.0).astype(jnp.float32)


def setup_inputs(seed: int = 0) -> dict:
    arg_keys = jax.random.split(jax.random.key(seed), 2)
    return {
        "coefficients": draw_coefficients(jax.random.fold_in(arg_keys[1], 71), 0),
    }


def reference(coefficients):
    margin = jnp.dot(coefficients.T.astype(jnp.float32), coefficients.astype(jnp.float32), precision=lax.Precision.HIGHEST, preferred_element_type=jnp.float32) / NG
    factor = jnp.linalg.cholesky(margin)
    solved = jax.scipy.linalg.solve_triangular(factor, coefficients.T, lower=True)
    return solved.T
```

```python
import jax
import jax.numpy as jnp
from jax import lax
from jax.experimental import pallas as pl
from jax.experimental.pallas import tpu as pltpu
from jax.sharding import PartitionSpec as P_

def bl(x, c):
    return jnp.broadcast_to(x[:, c:c+1], (8,128))
def bs(x, k):
    return jnp.broadcast_to(x[k:k+1, :], (8,128))

def leaf(W, nb=16):
    sub = lax.broadcasted_iota(jnp.int32, (8,128), 0)
    lane = lax.broadcasted_iota(jnp.int32, (8,128), 1)
    X = [jnp.where(lane == sub + 8*g, 1.0, 0.0).astype(jnp.float32) for g in range(nb)]
    W = list(W)
    out = []
    for g in range(nb):
        C = [[bl(W[h], 8*g+k) for k in range(8)] for h in range(g, nb)]
        fin = None
        for k in range(8):
            d = bs(C[0][k], k)
            r = lax.rsqrt(d)
            for c in C: c[k] = c[k]*r
            for j in range(k+1, 8):
                s = bs(C[0][k], j)
                for c in C: c[j] = c[j] - c[k]*s
            uW = bs(W[g], k)*r
            uX = bs(X[g], k)*r
            fin = uX if fin is None else jnp.where(sub == k, uX, fin)
            for i, c in enumerate(C):
                h = g+i
                if h == g and k == 7: continue
                W[h] = W[h] - c[k]*uW
                X[h] = X[h] - c[k]*uX
        out.append(fin)
    return out

NB=1024; R=160; LB=128; T=NB+R
F=jnp.float32; BF=jnp.bfloat16
NT=(((1,),(1,)),((),()))
def dnt(a,b): return lax.dot_general(a,b,NT,preferred_element_type=F)
def split(x):
    hi=x.astype(BF); lo=(x-hi.astype(F)).astype(BF)
    return hi,lo

def kern(g_ref, a_ref, q_ref, hi_ref, lo_ref, c_ref, xs_ref, d_ref, w_ref):
    hi_ref[...]=jnp.zeros_like(hi_ref); lo_ref[...]=jnp.zeros_like(lo_ref)
    c_ref[...]=jnp.zeros_like(c_ref); xs_ref[...]=jnp.zeros_like(xs_ref)
    def blk(p):
        return jnp.concatenate([g_ref[0,pl.ds(p*64,64),:],g_ref[1,pl.ds(p*64,64),:]],axis=0)
    d_ref[...]=blk(0)
    def splitx(x):
        xh,xl=split(x)
        return jnp.concatenate([xh,xl],axis=0)
    def mul3(ph,plo,r):
        t=dnt(ph,r)
        return t[:,:LB]+t[:,LB:]+dnt(plo,r[:LB])
    def body(kk,_):
        c0=pl.multiple_of(kk*LB,LB)
        off=kk*8-lax.shift_right_logical(kk*(kk-1),1)
        W=[d_ref[8*g:8*g+8,:] for g in range(16)]
        X=leaf(W)
        cp=pl.multiple_of(jnp.maximum(kk-1,0)*LB,LB)
        xs=xs_ref[...]
        for r0 in list(range(0,NB,LB))+[NB]:
            r1=min(r0+LB,T) if r0<NB else T
            ph,plo=split(c_ref[r0:r1,:])
            l=mul3(ph,plo,xs)
            h,lw=split(l)
            hi_ref[r0:r1,pl.ds(cp,LB)]=h; lo_ref[r0:r1,pl.ds(cp,LB)]=lw
            if r0==NB: q_ref[:,pl.ds(cp,LB)]=l
        rh=jnp.concatenate([hi_ref[pl.ds(c0,LB),:],lo_ref[pl.ds(c0,LB),:]],axis=0)
        for r0 in list(range(0,NB,LB))+[NB]:
            r1=min(r0+LB,T) if r0<NB else T
            m=blk(off+r0//LB-kk) if r0<NB else a_ref[:,pl.ds(c0,LB)]
            c_ref[r0:r1,:]=m-mul3(hi_ref[r0:r1,:],lo_ref[r0:r1,:],rh)
        kn=jnp.minimum(kk+1,7); n0=pl.multiple_of(kn*LB,LB)
        nh=hi_ref[pl.ds(n0,LB),:]; nl=lo_ref[pl.ds(n0,LB),:]
        dn=blk(kn*8-lax.shift_right_logical(kn*(kn-1),1))-mul3(nh,nl,jnp.concatenate([nh,nl],axis=0))
        xn=splitx(jnp.concatenate(X,axis=0))
        xs_ref[...]=xn
        ph,plo=split(c_ref[pl.ds(n0,LB),:])
        l=mul3(ph,plo,xn)
        h,lw=split(l)
        d_ref[...]=dn-mul3(h,lw,jnp.concatenate([h,lw],axis=0))
        return 0
    lax.fori_loop(0,8,body,0)
    ph,plo=split(c_ref[NB:T,:])
    q_ref[:,7*LB:]=mul3(ph,plo,xs_ref[...])

def chol(g,a):
    V=pl.BlockSpec(memory_space=pltpu.VMEM)
    return pl.pallas_call(kern, out_shape=jax.ShapeDtypeStruct((R,NB), F),
        in_specs=[V,V], out_specs=V, name="cholk",
        scratch_shapes=[pltpu.VMEM((T,NB),BF),pltpu.VMEM((T,NB),BF),pltpu.VMEM((T,LB),F),pltpu.VMEM((2*LB,LB),BF),pltpu.VMEM((LB,LB),F),pltpu.VMEM((LB,LB),F)],
        compiler_params=pltpu.CompilerParams(vmem_limit_bytes=40*1024*1024))(g,a)
NB=1024; R=160; LB=128; NG=20480
F=jnp.float32; BF=jnp.bfloat16
NN=(((1,),(0,)),((),()))
MESH=pl.DeviceIdType.MESH
def dnn(a,b): return lax.dot_general(a,b,NN,preferred_element_type=F)
def split(x):
    hi=x.astype(BF); lo=(x-hi.astype(F)).astype(BF)
    return hi,lo
ROWS=36*64; TH=ROWS//3; CH=TH//4; SC=CH//4
OFF=[j*8-j*(j-1)//2 for j in range(9)]

def comm_kern(a_ref, g_ref, b_ref, ah, al, th, tl, p_ref, r1, acc1, r2, acc2, r3, ssem, rsem):
    row=lax.axis_index("row"); col=lax.axis_index("col")
    core=lax.rem(row,2); crd=[lax.rem(col,4), lax.div(row,2), lax.div(col,4)]
    def dev(c,k): return (c[1]*2+k, c[2]*4+c[0])
    def peer(ax,o):
        c=list(crd); c[ax]=lax.rem(crd[ax]+o,4); return dev(c,core), c[ax]
    def src(ax,o): return lax.rem(crd[ax]+(4-o),4)
    partner=dev(crd,1-core)
    bar=pltpu.get_barrier_semaphore()
    pl.semaphore_signal(bar,inc=1,device_id=partner,device_id_type=MESH)
    for ax in range(3):
        for o in (1,2,3):
            pl.semaphore_signal(bar,inc=1,device_id=peer(ax,o)[0],device_id_type=MESH)
    pl.semaphore_wait(bar,10)
    sends=[]
    def rc(s,d,k,to):
        c=pltpu.make_async_remote_copy(src_ref=s,dst_ref=d,send_sem=ssem.at[k],recv_sem=rsem.at[k],device_id=to,device_id_type=MESH)
        return c
    ca=rc(a_ref,b_ref,0,partner); ca.start(); sends.append(ca)
    def put(x,r0):
        h,l=split(x)
        ah[r0:r0+R,:]=h; al[r0:r0+R,:]=l
    put(a_ref[...]*(1.0/NG),0) if False else put(a_ref[...],0)
    ca.wait_recv()
    put(b_ref[...],R)
    h64=pl.multiple_of(core*64,64)
    for i in range(8):
        th[i*LB:(i+1)*LB,:]=ah[:,i*LB:(i+1)*LB].T
        tl[i*LB:(i+1)*LB,:]=al[:,i*LB:(i+1)*LB].T
    lh=jnp.concatenate([th[pl.ds(i*LB+h64,64),:] for i in range(8)],axis=0)
    ll=jnp.concatenate([tl[pl.ds(i*LB+h64,64),:] for i in range(8)],axis=0)
    for j in range(8):
        bh=ah[:,j*LB:(j+1)*LB]; bl_=al[:,j*LB:(j+1)*LB]
        t=dnn(lh[64*j:],jnp.concatenate([bh,bl_],axis=1))
        p_ref[OFF[j]*64:OFF[j+1]*64,:]=(t[:,:LB]+t[:,LB:]+dnn(ll[64*j:],bh))*(1.0/NG)
    al8=lambda v: pl.multiple_of(v,16)
    def K(st,t,o): return 1+st*9+t*3+(o-1)
    A1=[0,1,2]; A2=[1,2,0]; A3=[2,0,1]
    c1={}
    for t in range(3):
        for o in (2,1,3):
            d,ci=peer(A1[t],o)
            c=rc(p_ref.at[pl.ds(al8(t*TH+ci*CH),CH),:], r1.at[t,o-1], K(0,t,o), d); c.start(); sends.append(c); c1[t,o]=c
    c2={}
    for t in range(3):
        for o in (1,2,3): c1[t,o].wait_recv()
        acc1[t]=p_ref[pl.ds(al8(t*TH+crd[A1[t]]*CH),CH),:]+r1[t,0]+r1[t,1]+r1[t,2]
        for o in (2,1,3):
            d,ci=peer(A2[t],o)
            c=rc(acc1.at[t,pl.ds(al8(ci*SC),SC),:], r2.at[t,o-1], K(1,t,o), d); c.start(); sends.append(c); c2[t,o]=c
    c3={}
    for t in range(3):
        for o in (1,2,3): c2[t,o].wait_recv()
        acc2[t]=acc1[t,pl.ds(al8(crd[A2[t]]*SC),SC),:]+r2[t,0]+r2[t,1]+r2[t,2]
        for o in (2,1,3):
            d,ci=peer(A3[t],o)
            c=rc(acc2.at[t], r3.at[t,o-1], K(2,t,o), d); c.start(); sends.append(c); c3[t,o]=c
    for t in range(3):
        for o in (1,2,3): c3[t,o].wait_recv()
        me=t*TH+crd[A1[t]]*CH+crd[A2[t]]*SC
        g_ref[core,pl.ds(al8(me),SC),:]=acc2[t]+r3[t,0]+r3[t,1]+r3[t,2]
        for o in (2,1,3):
            d,ci=peer(A2[t],o)
            s=g_ref.at[core,pl.ds(al8(me),SC),:]
            c=rc(s,s,K(3,t,o),d); c.start(); sends.append(c)
    for t in range(3):
        for o in (1,2,3):
            s=g_ref.at[core,pl.ds(al8(t*TH+crd[A1[t]]*CH+src(A2[t],o)*SC),SC),:]
            rc(s,s,K(3,t,o),partner).wait_recv()
        s=g_ref.at[core,pl.ds(al8(t*TH+crd[A1[t]]*CH),CH),:]
        for o in (2,1,3):
            d,ci=peer(A1[t],o)
            c=rc(s,s,K(4,t,o),d); c.start(); sends.append(c)
    for t in range(3):
        for o in (1,2,3):
            s=g_ref.at[core,pl.ds(al8(t*TH+src(A1[t],o)*CH),CH),:]
            rc(s,s,K(4,t,o),partner).wait_recv()
        s=g_ref.at[core,pl.ds(t*TH,TH),:]
        c=rc(s,s,46+t,partner); c.start(); sends.append(c)
    for t in range(3):
        s=g_ref.at[1-core,pl.ds(t*TH,TH),:]
        rc(s,s,46+t,partner).wait_recv()
    for c in sends: c.wait_send()

def gram_ar(a):
    V=pl.BlockSpec(memory_space=pltpu.VMEM)
    VM=pltpu.VMEM
    return pl.pallas_call(comm_kern, out_shape=jax.ShapeDtypeStruct((2,ROWS,LB),F),
        in_specs=[V], out_specs=V, name="gram_ar",
        scratch_shapes=[VM((R,NB),F),VM((2*R,NB),BF),VM((2*R,NB),BF),VM((NB,2*R),BF),VM((NB,2*R),BF),
            VM((ROWS,LB),F),VM((3,3,CH,LB),F),VM((3,CH,LB),F),VM((3,3,SC,LB),F),VM((3,SC,LB),F),VM((3,3,SC,LB),F),
            pltpu.SemaphoreType.DMA((49,)),pltpu.SemaphoreType.DMA((49,))],
        compiler_params=pltpu.CompilerParams(collective_id=0,has_side_effects=True,vmem_limit_bytes=40*1024*1024))(a)
def solution(mesh):
    def body(a):
        return chol(gram_ar(a), a)
    spec = P_(("row", "col"), None)
    return jax.shard_map(body, mesh=mesh, in_specs=spec, out_specs=spec, check_vma=False)
```

```python
import jax
import jax.numpy as jnp
from jax import lax
from jax.experimental import pallas as pl
from jax.experimental.pallas import tpu as pltpu
from jax.sharding import PartitionSpec as P_

def bl(x, c):
    return jnp.take_along_axis(x, jnp.full((8,128), c, jnp.int32), axis=1, mode='promise_in_bounds')
def bs(x, k):
    return jnp.broadcast_to(x[k:k+1, :], (8,128))

def leaf(W):
    BF=jnp.bfloat16; F=jnp.float32
    sub = lax.broadcasted_iota(jnp.int32, (8,128), 0)
    lane = lax.broadcasted_iota(jnp.int32, (8,128), 1)
    X = [jnp.where(lane == sub + 8*g, 1.0, 0.0).astype(F) for g in range(16)]
    W = list(W)
    out = [None]*16
    for G in range(8):
        g0, g1 = 2*G, 2*G+1
        nxt = list(range(2*G+2, min(2*G+6,16)))
        base = 16*G
        C = {}
        for k in range(16):
            for h in ([g0] if k < 8 else []) + [g1] + nxt:
                C[h, k] = bl(W[h], base+k)
        U = {}
        dn = None
        for k in range(16):
            own, i = (g0, k) if k < 8 else (g1, k-8)
            act = ([g0] if k < 8 else []) + [g1] + nxt
            d = bs(C[own, k], i) if dn is None else dn
            r = 1.0/d
            rs = lax.rsqrt(d)
            if k < 15:
                o2, i2 = (g0, k+1) if k+1 < 8 else (g1, k-7)
                cc = bs(C[o2, k], i2)
                dn = bs(C[o2, k+1], i2) - (cc*cc)*r
            m = {h: C[h, k]*r for h in act}
            for j in range(k+1, 16):
                s = bs(C[g0, k], j) if j < 8 else bs(C[g1, k], j-8)
                for h in ([g0] if j < 8 else []) + [g1] + nxt:
                    C[h, j] = C[h, j] - m[h]*s
            wr = bs(W[own], i)
            xr = bs(X[own], i)
            for h in act:
                if h == own and i == 7: continue
                W[h] = W[h] - m[h]*wr
                X[h] = X[h] - m[h]*xr
            fx = xr*rs
            out[own] = fx if i == 0 else jnp.where(sub == i, fx, out[own])
            if G < 5:
                fw = wr*rs
                U[own] = fw if i == 0 else jnp.where(sub == i, fw, U[own])
        if G < 5:
            u = jnp.concatenate([jnp.concatenate([U[g0], out[g0]], axis=1), jnp.concatenate([U[g1], out[g1]], axis=1)], axis=0)
            h = u.astype(BF); l = (u - h.astype(F)).astype(BF)
            a = jnp.concatenate([h[:, :128], h[:, :128], l[:, :128]], axis=0)
            b = jnp.concatenate([h, l, h], axis=0)
            upd = lax.dot_general(a, b, (((0,),(0,)),((),())), preferred_element_type=F)
            for q in range(2*G+6, 16):
                W[q] = W[q] - upd[8*q:8*q+8, :128]
                X[q] = X[q] - upd[8*q:8*q+8, 128:]
    return out

NB=1024; R=160; LB=128; T=NB+R
F=jnp.float32; BF=jnp.bfloat16
NT=(((1,),(1,)),((),()))
def dnt(a,b): return lax.dot_general(a,b,NT,preferred_element_type=F)
def split(x):
    hi=x.astype(BF); lo=(x-hi.astype(F)).astype(BF)
    return hi,lo

def kern(g_ref, a_ref, q_ref, hi_ref, lo_ref, c_ref, xs_ref, d_ref, w_ref):
    hi_ref[...]=jnp.zeros_like(hi_ref); lo_ref[...]=jnp.zeros_like(lo_ref)
    c_ref[...]=jnp.zeros_like(c_ref); xs_ref[...]=jnp.zeros_like(xs_ref)
    def blk(p):
        return jnp.concatenate([g_ref[0,pl.ds(p*64,64),:],g_ref[1,pl.ds(p*64,64),:]],axis=0)
    d_ref[...]=blk(0)
    def splitx(x):
        xh,xl=split(x)
        return jnp.concatenate([xh,xl],axis=0)
    def mul3(ph,plo,r):
        t=dnt(ph,r)
        return t[:,:LB]+t[:,LB:]+dnt(plo,r[:LB])
    def mk(rlo,K):
      def body(kk,_):
        c0=pl.multiple_of(kk*LB,LB)
        off=kk*8-lax.shift_right_logical(kk*(kk-1),1)
        W=[d_ref[8*g:8*g+8,:] for g in range(16)]
        X=leaf(W)
        cp=pl.multiple_of(jnp.maximum(kk-1,0)*LB,LB)
        xs=xs_ref[...]
        ph,plo=split(c_ref[rlo:T,:])
        l=mul3(ph,plo,xs)
        h,lw=split(l)
        hi_ref[rlo:T,pl.ds(cp,LB)]=h; lo_ref[rlo:T,pl.ds(cp,LB)]=lw
        q_ref[:,pl.ds(cp,LB)]=l[NB-rlo:]
        rh=jnp.concatenate([hi_ref[pl.ds(c0,LB),0:K],lo_ref[pl.ds(c0,LB),0:K]],axis=0)
        u=mul3(hi_ref[rlo:T,0:K],lo_ref[rlo:T,0:K],rh)
        for r0 in range(rlo,NB,LB):
            c_ref[r0:r0+LB,:]=blk(off+r0//LB-kk)-u[r0-rlo:r0-rlo+LB]
        c_ref[NB:T,:]=a_ref[:,pl.ds(c0,LB)]-u[NB-rlo:]
        kn=jnp.minimum(kk+1,7); n0=pl.multiple_of(kn*LB,LB)
        nh=hi_ref[pl.ds(n0,LB),0:K]; nl=lo_ref[pl.ds(n0,LB),0:K]
        dn=blk(kn*8-lax.shift_right_logical(kn*(kn-1),1))-mul3(nh,nl,jnp.concatenate([nh,nl],axis=0))
        xn=splitx(jnp.concatenate(X,axis=0))
        xs_ref[...]=xn
        ph,plo=split(c_ref[pl.ds(n0,LB),:])
        l=mul3(ph,plo,xn)
        h,lw=split(l)
        d_ref[...]=dn-mul3(h,lw,jnp.concatenate([h,lw],axis=0))
        return 0
      return body
    lax.fori_loop(0,4,mk(0,512),0)
    lax.fori_loop(4,8,mk(512,1024),0)
    ph,plo=split(c_ref[NB:T,:])
    q_ref[:,7*LB:]=mul3(ph,plo,xs_ref[...])

def chol(g,a):
    V=pl.BlockSpec(memory_space=pltpu.VMEM)
    return pl.pallas_call(kern, out_shape=jax.ShapeDtypeStruct((R,NB), F),
        in_specs=[V,V], out_specs=V, name="cholk",
        scratch_shapes=[pltpu.VMEM((T,NB),BF),pltpu.VMEM((T,NB),BF),pltpu.VMEM((T,LB),F),pltpu.VMEM((2*LB,LB),BF),pltpu.VMEM((LB,LB),F),pltpu.VMEM((LB,LB),F)],
        compiler_params=pltpu.CompilerParams(vmem_limit_bytes=40*1024*1024))(g,a)
NB=1024; R=160; LB=128; NG=20480
F=jnp.float32; BF=jnp.bfloat16
NN=(((1,),(0,)),((),()))
MESH=pl.DeviceIdType.MESH
def dnn(a,b): return lax.dot_general(a,b,NN,preferred_element_type=F)
def split(x):
    hi=x.astype(BF); lo=(x-hi.astype(F)).astype(BF)
    return hi,lo
ROWS=36*64; TH=ROWS//3; CH=TH//4; SC=CH//4
OFF=[j*8-j*(j-1)//2 for j in range(9)]

def comm_kern(a_ref, g_ref, b_ref, ah, al, th, tl, p_ref, r1, acc1, r2, acc2, r3, ssem, rsem):
    row=lax.axis_index("row"); col=lax.axis_index("col")
    core=lax.rem(row,2); crd=[lax.rem(col,4), lax.div(row,2), lax.div(col,4)]
    def dev(c,k): return (c[1]*2+k, c[2]*4+c[0])
    def peer(ax,o):
        c=list(crd); c[ax]=lax.rem(crd[ax]+o,4); return dev(c,core), c[ax]
    def src(ax,o): return lax.rem(crd[ax]+(4-o),4)
    partner=dev(crd,1-core)
    bar=pltpu.get_barrier_semaphore()
    pl.semaphore_signal(bar,inc=1,device_id=partner,device_id_type=MESH)
    for ax in range(3):
        for o in (1,2,3):
            pl.semaphore_signal(bar,inc=1,device_id=peer(ax,o)[0],device_id_type=MESH)
    pl.semaphore_wait(bar,10)
    sends=[]
    def rc(s,d,k,to):
        c=pltpu.make_async_remote_copy(src_ref=s,dst_ref=d,send_sem=ssem.at[k],recv_sem=rsem.at[k],device_id=to,device_id_type=MESH)
        return c
    ca=rc(a_ref,b_ref,0,partner); ca.start(); sends.append(ca)
    def put(x,r0):
        h,l=split(x)
        ah[r0:r0+R,:]=h; al[r0:r0+R,:]=l
    put(a_ref[...]*(1.0/NG),0) if False else put(a_ref[...],0)
    ca.wait_recv()
    put(b_ref[...],R)
    h64=pl.multiple_of(core*64,64)
    for i in range(8):
        th[i*LB:(i+1)*LB,:]=ah[:,i*LB:(i+1)*LB].T
        tl[i*LB:(i+1)*LB,:]=al[:,i*LB:(i+1)*LB].T
    lh=jnp.concatenate([th[pl.ds(i*LB+h64,64),:] for i in range(8)],axis=0)
    ll=jnp.concatenate([tl[pl.ds(i*LB+h64,64),:] for i in range(8)],axis=0)
    for j in range(8):
        bh=ah[:,j*LB:(j+1)*LB]; bl_=al[:,j*LB:(j+1)*LB]
        t=dnn(lh[64*j:],jnp.concatenate([bh,bl_],axis=1))
        p_ref[OFF[j]*64:OFF[j+1]*64,:]=(t[:,:LB]+t[:,LB:]+dnn(ll[64*j:],bh))*(1.0/NG)
    al8=lambda v: pl.multiple_of(v,16)
    def K(st,t,o): return 1+st*9+t*3+(o-1)
    A1=[0,1,2]; A2=[1,2,0]; A3=[2,0,1]
    c1={}
    for t in range(3):
        for o in (2,1,3):
            d,ci=peer(A1[t],o)
            c=rc(p_ref.at[pl.ds(al8(t*TH+ci*CH),CH),:], r1.at[t,o-1], K(0,t,o), d); c.start(); sends.append(c); c1[t,o]=c
    c2={}
    for t in range(3):
        for o in (1,2,3): c1[t,o].wait_recv()
        acc1[t]=p_ref[pl.ds(al8(t*TH+crd[A1[t]]*CH),CH),:]+r1[t,0]+r1[t,1]+r1[t,2]
        for o in (2,1,3):
            d,ci=peer(A2[t],o)
            c=rc(acc1.at[t,pl.ds(al8(ci*SC),SC),:], r2.at[t,o-1], K(1,t,o), d); c.start(); sends.append(c); c2[t,o]=c
    c3={}
    for t in range(3):
        for o in (1,2,3): c2[t,o].wait_recv()
        acc2[t]=acc1[t,pl.ds(al8(crd[A2[t]]*SC),SC),:]+r2[t,0]+r2[t,1]+r2[t,2]
        for o in (2,1,3):
            d,ci=peer(A3[t],o)
            c=rc(acc2.at[t], r3.at[t,o-1], K(2,t,o), d); c.start(); sends.append(c); c3[t,o]=c
    for t in range(3):
        for o in (1,2,3): c3[t,o].wait_recv()
        me=t*TH+crd[A1[t]]*CH+crd[A2[t]]*SC
        g_ref[core,pl.ds(al8(me),SC),:]=acc2[t]+r3[t,0]+r3[t,1]+r3[t,2]
        for o in (2,1,3):
            d,ci=peer(A2[t],o)
            s=g_ref.at[core,pl.ds(al8(me),SC),:]
            c=rc(s,s,K(3,t,o),d); c.start(); sends.append(c)
    for t in range(3):
        for o in (1,2,3):
            s=g_ref.at[core,pl.ds(al8(t*TH+crd[A1[t]]*CH+src(A2[t],o)*SC),SC),:]
            rc(s,s,K(3,t,o),partner).wait_recv()
        s=g_ref.at[core,pl.ds(al8(t*TH+crd[A1[t]]*CH),CH),:]
        for o in (2,1,3):
            d,ci=peer(A1[t],o)
            c=rc(s,s,K(4,t,o),d); c.start(); sends.append(c)
    for t in range(3):
        for o in (1,2,3):
            s=g_ref.at[core,pl.ds(al8(t*TH+src(A1[t],o)*CH),CH),:]
            rc(s,s,K(4,t,o),partner).wait_recv()
        s=g_ref.at[core,pl.ds(t*TH,TH),:]
        c=rc(s,s,46+t,partner); c.start(); sends.append(c)
    for t in range(3):
        s=g_ref.at[1-core,pl.ds(t*TH,TH),:]
        rc(s,s,46+t,partner).wait_recv()
    for c in sends: c.wait_send()

def gram_ar(a):
    V=pl.BlockSpec(memory_space=pltpu.VMEM)
    VM=pltpu.VMEM
    return pl.pallas_call(comm_kern, out_shape=jax.ShapeDtypeStruct((2,ROWS,LB),F),
        in_specs=[V], out_specs=V, name="gram_ar",
        scratch_shapes=[VM((R,NB),F),VM((2*R,NB),BF),VM((2*R,NB),BF),VM((NB,2*R),BF),VM((NB,2*R),BF),
            VM((ROWS,LB),F),VM((3,3,CH,LB),F),VM((3,CH,LB),F),VM((3,3,SC,LB),F),VM((3,SC,LB),F),VM((3,3,SC,LB),F),
            pltpu.SemaphoreType.DMA((49,)),pltpu.SemaphoreType.DMA((49,))],
        compiler_params=pltpu.CompilerParams(collective_id=0,has_side_effects=True,vmem_limit_bytes=40*1024*1024))(a)
def solution(mesh):
    def body(a):
        return chol(gram_ar(a), a)
    spec = P_(("row", "col"), None)
    return jax.shard_map(body, mesh=mesh, in_specs=spec, out_specs=spec, check_vma=False)
```

```python
import jax
import jax.numpy as jnp
from jax import lax
from jax.experimental import pallas as pl
from jax.experimental.pallas import tpu as pltpu
from jax.sharding import PartitionSpec as P_

def bl(x, c):
    return jnp.take_along_axis(x, jnp.full((8,128), c, jnp.int32), axis=1, mode='promise_in_bounds')
def bs(x, k):
    return jnp.broadcast_to(x[k:k+1, :], (8,128))

def leaf(W):
    BF=jnp.bfloat16; F=jnp.float32
    sub = lax.broadcasted_iota(jnp.int32, (8,128), 0)
    lane = lax.broadcasted_iota(jnp.int32, (8,128), 1)
    X = [jnp.where(lane == sub + 8*g, 1.0, 0.0).astype(F) for g in range(16)]
    W = list(W)
    out = [None]*16
    for G in range(8):
        g0, g1 = 2*G, 2*G+1
        nxt = list(range(2*G+2, min(2*G+6,16)))
        base = 16*G
        C = {}
        for k in range(16):
            for h in ([g0] if k < 8 else []) + [g1] + nxt:
                C[h, k] = bl(W[h], base+k)
        U = {}
        dn = None
        for k in range(16):
            own, i = (g0, k) if k < 8 else (g1, k-8)
            act = ([g0] if k < 8 else []) + [g1] + nxt
            d = bs(C[own, k], i) if dn is None else dn
            r = 1.0/d
            rs = lax.rsqrt(d)
            if k < 15:
                o2, i2 = (g0, k+1) if k+1 < 8 else (g1, k-7)
                cc = bs(C[o2, k], i2)
                dn = bs(C[o2, k+1], i2) - (cc*cc)*r
            m = {h: C[h, k]*r for h in act}
            for j in range(k+1, 16):
                s = bs(C[g0, k], j) if j < 8 else bs(C[g1, k], j-8)
                for h in ([g0] if j < 8 else []) + [g1] + nxt:
                    C[h, j] = C[h, j] - m[h]*s
            wr = bs(W[own], i)
            xr = bs(X[own], i)
            for h in act:
                if h == own and i == 7: continue
                W[h] = W[h] - m[h]*wr
                X[h] = X[h] - m[h]*xr
            fx = xr*rs
            out[own] = fx if i == 0 else jnp.where(sub == i, fx, out[own])
            if G < 5:
                fw = wr*rs
                U[own] = fw if i == 0 else jnp.where(sub == i, fw, U[own])
        if G < 5:
            u = jnp.concatenate([jnp.concatenate([U[g0], out[g0]], axis=1), jnp.concatenate([U[g1], out[g1]], axis=1)], axis=0)
            h = u.astype(BF); l = (u - h.astype(F)).astype(BF)
            a = jnp.concatenate([h[:, :128], h[:, :128], l[:, :128]], axis=0)
            b = jnp.concatenate([h, l, h], axis=0)
            upd = lax.dot_general(a, b, (((0,),(0,)),((),())), preferred_element_type=F)
            for q in range(2*G+6, 16):
                W[q] = W[q] - upd[8*q:8*q+8, :128]
                X[q] = X[q] - upd[8*q:8*q+8, 128:]
    return out


NB=1024; R=160; LB=128; T=NB+R; NG=20480
F=jnp.float32; BF=jnp.bfloat16
NT=(((1,),(1,)),((),())); NN=(((1,),(0,)),((),()))
MESH=pl.DeviceIdType.MESH
def dnt(a,b): return lax.dot_general(a,b,NT,preferred_element_type=F)
def dnn(a,b): return lax.dot_general(a,b,NN,preferred_element_type=F)
def split(x):
    hi=x.astype(BF); lo=(x-hi.astype(F)).astype(BF)
    return hi,lo
ROWS=36*64; PH=ROWS//3; TH=PH//3; CH=TH//4; SC=CH//4
OFF=[j*8-j*(j-1)//2 for j in range(9)]

def kernel(a_ref, q_ref, g_ref, b_ref, ah, al, th, tl, p_ref, r1, acc1, r2, acc2, r3,
           hi_ref, lo_ref, c_ref, xs_ref, d_ref, ssem, rsem):
    row=lax.axis_index("row"); col=lax.axis_index("col")
    core=lax.rem(row,2); crd=[lax.rem(col,4), lax.div(row,2), lax.div(col,4)]
    def dev(c,k): return (c[1]*2+k, c[2]*4+c[0])
    def peer(ax,o):
        c=list(crd); c[ax]=lax.rem(crd[ax]+o,4); return dev(c,core), c[ax]
    def src(ax,o): return lax.rem(crd[ax]+(4-o),4)
    partner=dev(crd,1-core)
    bar=pltpu.get_barrier_semaphore()
    pl.semaphore_signal(bar,inc=1,device_id=partner,device_id_type=MESH)
    for ax in range(3):
        for o in (1,2,3):
            pl.semaphore_signal(bar,inc=1,device_id=peer(ax,o)[0],device_id_type=MESH)
    sends=[]
    def rc(s,d,k,to):
        return pltpu.make_async_remote_copy(src_ref=s,dst_ref=d,send_sem=ssem.at[k],recv_sem=rsem.at[k],device_id=to,device_id_type=MESH)
    def go(s,d,k,to):
        c=rc(s,d,k,to); c.start(); sends.append(c); return c
    def prep(x,n):
        h,l=split(x)
        ah[n]=h; al[n]=l
        for i in range(8):
            th[n,i*LB:(i+1)*LB,:]=h[:,i*LB:(i+1)*LB].T
            tl[n,i*LB:(i+1)*LB,:]=l[:,i*LB:(i+1)*LB].T
    h64=pl.multiple_of(core*64,64)
    def gram(n,js):
        lh=jnp.concatenate([th[n,pl.ds(i*LB+h64,64),:] for i in range(js[0],8)],axis=0)
        ll=jnp.concatenate([tl[n,pl.ds(i*LB+h64,64),:] for i in range(js[0],8)],axis=0)
        for j in js:
            bh=ah[n,:,j*LB:(j+1)*LB]; bl_=al[n,:,j*LB:(j+1)*LB]
            z=64*(j-js[0])
            t=dnn(lh[z:],jnp.concatenate([bh,bl_],axis=1))
            u=t[:,:LB]+t[:,LB:]+dnn(ll[z:],bh)
            s=slice(OFF[j]*64,OFF[j+1]*64)
            if n==0: p_ref[s,:]=u
            else: p_ref[s,:]=(p_ref[s,:]+u)*(1.0/NG)
    pl.semaphore_wait(bar,10)
    ca=go(a_ref,b_ref,0,partner)
    prep(a_ref[...],0)
    gram(0,list(range(8)))
    ca.wait_recv()
    prep(b_ref[...],1)
    al8=lambda v: pl.multiple_of(v,16)
    def K(f,st,t,o): return 1+(f*5+st)*9+t*3+(o-1)
    A1=[0,1,2]; A2=[1,2,0]; A3=[2,0,1]
    OS=(2,1,3); C={}
    def st1(f):
        for t in range(3):
            for o in OS:
                d,ci=peer(A1[t],o)
                C[f,1,t,o]=go(p_ref.at[pl.ds(al8(f*PH+t*TH+ci*CH),CH),:], r1.at[f,t,o-1], K(f,0,t,o), d)
    def st2(f):
        for t in range(3):
            for o in OS: C[f,1,t,o].wait_recv()
            acc1[f,t]=p_ref[pl.ds(al8(f*PH+t*TH+crd[A1[t]]*CH),CH),:]+r1[f,t,0]+r1[f,t,1]+r1[f,t,2]
            for o in OS:
                d,ci=peer(A2[t],o)
                C[f,2,t,o]=go(acc1.at[f,t,pl.ds(al8(ci*SC),SC),:], r2.at[f,t,o-1], K(f,1,t,o), d)
    def st3(f):
        for t in range(3):
            for o in OS: C[f,2,t,o].wait_recv()
            acc2[f,t]=acc1[f,t,pl.ds(al8(crd[A2[t]]*SC),SC),:]+r2[f,t,0]+r2[f,t,1]+r2[f,t,2]
            for o in OS:
                d,ci=peer(A3[t],o)
                C[f,3,t,o]=go(acc2.at[f,t], r3.at[f,t,o-1], K(f,2,t,o), d)
    def mine(f,t): return f*PH+t*TH+crd[A1[t]]*CH
    def st4(f):
        for t in range(3):
            for o in OS: C[f,3,t,o].wait_recv()
            me=al8(mine(f,t)+crd[A2[t]]*SC)
            g_ref[core,pl.ds(me,SC),:]=acc2[f,t]+r3[f,t,0]+r3[f,t,1]+r3[f,t,2]
            s=g_ref.at[core,pl.ds(me,SC),:]
            for o in OS: go(s,s,K(f,3,t,o),peer(A2[t],o)[0])
    def st5(f):
        for t in range(3):
            for o in OS:
                s=g_ref.at[core,pl.ds(al8(mine(f,t)+src(A2[t],o)*SC),SC),:]
                rc(s,s,K(f,3,t,o),partner).wait_recv()
            s=g_ref.at[core,pl.ds(al8(mine(f,t)),CH),:]
            for o in OS: go(s,s,K(f,4,t,o),peer(A1[t],o)[0])
    def c6(f,t,k):
        s=g_ref.at[k,pl.ds(f*PH+t*TH,TH),:]
        return rc(s,s,136+f*3+t,partner)
    def st6(f,keep=True):
        for t in range(3):
            for o in OS:
                s=g_ref.at[core,pl.ds(al8(f*PH+t*TH+src(A1[t],o)*CH),CH),:]
                rc(s,s,K(f,4,t,o),partner).wait_recv()
            c6(f,t,core).start()
    def fin(f):
        for t in range(3): c6(f,t,1-core).wait_recv()
    gram(1,[0,1])
    st1(0)
    gram(1,[2,3,4,5,6,7])
    st1(1); st2(0); st1(2)
    def comm_rest():
        st3(0); st2(1)
        st4(0); st3(1); st2(2)
        st5(0); st4(1); st3(2)
        st6(0); st5(1); st4(2)
        fin(0); st6(1); st5(2)
    def hook(kk):
        @pl.when(kk==1)
        def _():
            fin(1); st6(2)
        @pl.when(kk==3)
        def _():
            fin(2)
    hi_ref[...]=jnp.zeros_like(hi_ref); lo_ref[...]=jnp.zeros_like(lo_ref)
    c_ref[...]=jnp.zeros_like(c_ref); xs_ref[...]=jnp.zeros_like(xs_ref)
    def blk(p):
        return jnp.concatenate([g_ref[0,pl.ds(p*64,64),:],g_ref[1,pl.ds(p*64,64),:]],axis=0)
    def splitx(x):
        xh,xl=split(x)
        return jnp.concatenate([xh,xl],axis=0)
    def mul3(ph,plo,r):
        t=dnt(ph,r)
        return t[:,:LB]+t[:,LB:]+dnt(plo,r[:LB])
    def mk(rlo,K):
      def body(kk,_):
        if rlo==0: hook(kk)
        c0=pl.multiple_of(kk*LB,LB)
        off=kk*8-lax.shift_right_logical(kk*(kk-1),1)
        W=[d_ref[8*g:8*g+8,:] for g in range(16)]
        X=leaf(W)
        cp=pl.multiple_of(jnp.maximum(kk-1,0)*LB,LB)
        xs=xs_ref[...]
        ph,plo=split(c_ref[rlo:T,:])
        l=mul3(ph,plo,xs)
        h,lw=split(l)
        hi_ref[rlo:T,pl.ds(cp,LB)]=h; lo_ref[rlo:T,pl.ds(cp,LB)]=lw
        q_ref[:,pl.ds(cp,LB)]=l[NB-rlo:]
        rh=jnp.concatenate([hi_ref[pl.ds(c0,LB),0:K],lo_ref[pl.ds(c0,LB),0:K]],axis=0)
        u=mul3(hi_ref[rlo:T,0:K],lo_ref[rlo:T,0:K],rh)
        for r0 in range(rlo,NB,LB):
            c_ref[r0:r0+LB,:]=blk(off+r0//LB-kk)-u[r0-rlo:r0-rlo+LB]
        c_ref[NB:T,:]=a_ref[:,pl.ds(c0,LB)]-u[NB-rlo:]
        kn=jnp.minimum(kk+1,7); n0=pl.multiple_of(kn*LB,LB)
        nh=hi_ref[pl.ds(n0,LB),0:K]; nl=lo_ref[pl.ds(n0,LB),0:K]
        dn=blk(kn*8-lax.shift_right_logical(kn*(kn-1),1))-mul3(nh,nl,jnp.concatenate([nh,nl],axis=0))
        xn=splitx(jnp.concatenate(X,axis=0))
        xs_ref[...]=xn
        ph,plo=split(c_ref[pl.ds(n0,LB),:])
        l=mul3(ph,plo,xn)
        h,lw=split(l)
        d_ref[...]=dn-mul3(h,lw,jnp.concatenate([h,lw],axis=0))
        return 0
      return body
    comm_rest()
    d_ref[...]=blk(0)
    lax.fori_loop(0,4,mk(0,512),0)
    lax.fori_loop(4,8,mk(512,1024),0)
    ph,plo=split(c_ref[NB:T,:])
    q_ref[:,7*LB:]=mul3(ph,plo,xs_ref[...])

    for c in sends: c.wait_send()
    for f in range(3):
        for t in range(3): c6(f,t,core).wait_send()

def solution(mesh):
    VM=pltpu.VMEM
    V=pl.BlockSpec(memory_space=VM)
    def body(a):
        return pl.pallas_call(kernel, out_shape=jax.ShapeDtypeStruct((R,NB),F),
            in_specs=[V], out_specs=V, name="ortho",
            scratch_shapes=[VM((2,ROWS,LB),F),VM((R,NB),F),VM((2,R,NB),BF),VM((2,R,NB),BF),VM((2,NB,R),BF),VM((2,NB,R),BF),
                VM((ROWS,LB),F),VM((3,3,3,CH,LB),F),VM((3,3,CH,LB),F),VM((3,3,3,SC,LB),F),VM((3,3,SC,LB),F),VM((3,3,3,SC,LB),F),
                VM((T,NB),BF),VM((T,NB),BF),VM((T,LB),F),VM((2*LB,LB),BF),VM((LB,LB),F),
                pltpu.SemaphoreType.DMA((145,)),pltpu.SemaphoreType.DMA((145,))],
            compiler_params=pltpu.CompilerParams(collective_id=0,has_side_effects=True,vmem_limit_bytes=48*1024*1024))(a)
    spec = P_(("row", "col"), None)
    return jax.shard_map(body, mesh=mesh, in_specs=spec, out_specs=spec, check_vma=False)
```

```python
import jax
import jax.numpy as jnp
from jax import lax
from jax.experimental import pallas as pl
from jax.experimental.pallas import tpu as pltpu
from jax.sharding import PartitionSpec as P_

def bl(x, c):
    return jnp.take_along_axis(x, jnp.full((8,128), c, jnp.int32), axis=1, mode='promise_in_bounds')
def bs(x, k):
    return jnp.broadcast_to(x[k:k+1, :], (8,128))

def leaf(W, near=4, full=2):
    BF=jnp.bfloat16; F=jnp.float32
    sub = lax.broadcasted_iota(jnp.int32, (8,128), 0)
    lane = lax.broadcasted_iota(jnp.int32, (8,128), 1)
    W = list(W)
    out = [None]*16
    rv = jnp.zeros((8,128), F)
    for G in range(8):
        g0, g1 = 2*G, 2*G+1
        nf = list(range(2*G+2, min(2*G+2+full,16)))
        nh = list(range(2*G+2+full, min(2*G+2+near,16)))
        base = 16*G
        far = 2*G+2+near < 16
        C = {}
        for k in range(16):
            for h in ([g0] if k < 8 else []) + [g1] + nf + (nh if k < 8 else []):
                C[h, k] = bl(W[h], base+k)
        U = {}
        dn = None
        for k in range(16):
            if k == 8:
                for h in nh:
                    for kk in range(8, 16): C[h, kk] = bl(W[h], base+kk)
            own, i = (g0, k) if k < 8 else (g1, k-8)
            act = ([g0] if k < 8 else []) + [g1] + nf + nh
            d = bs(C[own, k], i) if dn is None else dn
            r = 1.0/d
            rs = lax.rsqrt(d)
            if k < 15:
                o2, i2 = (g0, k+1) if k+1 < 8 else (g1, k-7)
                cc = bs(C[o2, k], i2)
                dn = bs(C[o2, k+1], i2) - (cc*cc)*r
            m = {h: C[h, k]*r for h in act}
            for j in range(k+1, 16):
                s = bs(C[g0, k], j) if j < 8 else bs(C[g1, k], j-8)
                for h in ([g0] if j < 8 else []) + [g1] + nf + (nh if (j < 8 or k >= 8) else []):
                    C[h, j] = C[h, j] - m[h]*s
            wr = bs(W[own], i)
            hot = lane == base+k
            wr2 = jnp.where(hot, wr+wr, wr)
            for h in act:
                if h == own and i == 7: continue
                W[h] = W[h] - m[h]*wr2
            fx = wr*rs
            out[own] = fx if i == 0 else jnp.where(sub == i, fx, out[own])
            rv = jnp.where(hot, r, rv)
        if far:
            u = jnp.concatenate([out[g0], out[g1]], axis=0)
            cl = lax.broadcasted_iota(jnp.int32, (16,128), 1)
            rw = lax.broadcasted_iota(jnp.int32, (16,128), 0)
            ub = jnp.where((cl <= base+rw) | (cl >= base+16), u, 0.0)
            h = ub.astype(BF); l = (ub - h.astype(F)).astype(BF)
            ur = jnp.where(cl >= base+16, u, 0.0)
            hr = ur.astype(BF); lr = (ur - hr.astype(F)).astype(BF)
            a = jnp.concatenate([hr, hr, lr], axis=0)
            b = jnp.concatenate([h, l, h], axis=0)
            upd = lax.dot_general(a, b, (((0,),(0,)),((),())), preferred_element_type=F)
            keep = (lane < base) | (lane >= base+16)
            for q in range(2*G+2+near, 16):
                W[q] = jnp.where(keep, W[q], 0.0) - upd[8*q:8*q+8, :]
    res = []
    for g in range(16):
        res.append(jnp.where(lane <= sub + 8*g, out[g]*rv, 0.0))
    return res

NB=1024; R=160; LB=128; T=NB+R; NG=20480
F=jnp.float32; BF=jnp.bfloat16
NT=(((1,),(1,)),((),())); NN=(((1,),(0,)),((),()))
MESH=pl.DeviceIdType.MESH
def dnt(a,b): return lax.dot_general(a,b,NT,preferred_element_type=F)
def dnn(a,b): return lax.dot_general(a,b,NN,preferred_element_type=F)
def split(x):
    hi=x.astype(BF); lo=(x-hi.astype(F)).astype(BF)
    return hi,lo
ROWS=36*64; PH=ROWS//3; TH=PH//3; CH=TH//4; SC=CH//4
OFF=[j*8-j*(j-1)//2 for j in range(9)]

def kernel(x_ref, q_ref, a_ref, g_ref, b_ref, ah, al, th, tl, p_ref, r1, acc1, r2, acc2, r3,
           hi_ref, lo_ref, c_ref, xs_ref, d_ref, ssem, rsem, lsem):
    row=lax.axis_index("row"); col=lax.axis_index("col")
    core=lax.rem(row,2); crd=[lax.rem(col,4), lax.div(row,2), lax.div(col,4)]
    def dev(c,k): return (c[1]*2+k, c[2]*4+c[0])
    def peer(ax,o):
        c=list(crd); c[ax]=lax.rem(crd[ax]+o,4); return dev(c,core), c[ax]
    def src(ax,o): return lax.rem(crd[ax]+(4-o),4)
    partner=dev(crd,1-core)
    bar=pltpu.get_barrier_semaphore()
    pl.semaphore_signal(bar,inc=1,device_id=partner,device_id_type=MESH)
    for ax in range(3):
        for o in (1,2,3):
            pl.semaphore_signal(bar,inc=1,device_id=peer(ax,o)[0],device_id_type=MESH)
    sends=[]
    def rc(s,d,k,to):
        return pltpu.make_async_remote_copy(src_ref=s,dst_ref=d,send_sem=ssem.at[k],recv_sem=rsem.at[k],device_id=to,device_id_type=MESH)
    def go(s,d,k,to):
        c=rc(s,d,k,to); c.start(); sends.append(c); return c
    def prep(x,n):
        h,l=split(x)
        ah[n]=h; al[n]=l
        for i in range(8):
            th[n,i*LB:(i+1)*LB,:]=h[:,i*LB:(i+1)*LB].T
            tl[n,i*LB:(i+1)*LB,:]=l[:,i*LB:(i+1)*LB].T
    h64=pl.multiple_of(core*64,64)
    def gram(n,js):
        lh=jnp.concatenate([th[n,pl.ds(i*LB+h64,64),:] for i in range(js[0],8)],axis=0)
        ll=jnp.concatenate([tl[n,pl.ds(i*LB+h64,64),:] for i in range(js[0],8)],axis=0)
        for j in js:
            bh=ah[n,:,j*LB:(j+1)*LB]; bl_=al[n,:,j*LB:(j+1)*LB]
            z=64*(j-js[0])
            t=dnn(lh[z:],jnp.concatenate([bh,bl_],axis=1))
            u=t[:,:LB]+t[:,LB:]+dnn(ll[z:],bh)
            s=slice(OFF[j]*64,OFF[j+1]*64)
            if n==0: p_ref[s,:]=u
            else: p_ref[s,:]=(p_ref[s,:]+u)*(1.0/NG)
    ld=pltpu.make_async_copy(x_ref,a_ref,lsem); ld.start()
    hi_ref[...]=jnp.zeros_like(hi_ref); lo_ref[...]=jnp.zeros_like(lo_ref)
    c_ref[...]=jnp.zeros_like(c_ref); xs_ref[...]=jnp.zeros_like(xs_ref)
    ld.wait()
    prep(a_ref[...],0)
    pl.semaphore_wait(bar,10)
    ca=go(a_ref,b_ref,0,partner)
    gram(0,list(range(8)))
    ca.wait_recv()
    prep(b_ref[...],1)
    al8=lambda v: pl.multiple_of(v,8)
    def K(f,st,t,o): return 1+(f*5+st)*9+t*3+(o-1)
    A1=[0,1,2]; A2=[1,2,0]; A3=[2,0,1]
    OS=(2,1,3); C={}
    def st1(f):
        for t in range(3):
            for o in OS:
                d,ci=peer(A1[t],o)
                C[f,1,t,o]=go(p_ref.at[pl.ds(al8(f*PH+t*TH+ci*CH),CH),:], r1.at[f,t,o-1], K(f,0,t,o), d)
    def st2(f):
        for t in range(3):
            for o in OS: C[f,1,t,o].wait_recv()
            acc1[f,t]=p_ref[pl.ds(al8(f*PH+t*TH+crd[A1[t]]*CH),CH),:]+r1[f,t,0]+r1[f,t,1]+r1[f,t,2]
            for o in OS:
                d,ci=peer(A2[t],o)
                C[f,2,t,o]=go(acc1.at[f,t,pl.ds(al8(ci*SC),SC),:], r2.at[f,t,o-1], K(f,1,t,o), d)
    def st3(f):
        for t in range(3):
            for o in OS: C[f,2,t,o].wait_recv()
            acc2[f,t]=acc1[f,t,pl.ds(al8(crd[A2[t]]*SC),SC),:]+r2[f,t,0]+r2[f,t,1]+r2[f,t,2]
            for o in OS:
                d,ci=peer(A3[t],o)
                C[f,3,t,o]=go(acc2.at[f,t], r3.at[f,t,o-1], K(f,2,t,o), d)
    def mine(f,t): return f*PH+t*TH+crd[A1[t]]*CH
    def st4(f):
        for t in range(3):
            for o in OS: C[f,3,t,o].wait_recv()
            me=al8(mine(f,t)+crd[A2[t]]*SC)
            g_ref[core,pl.ds(me,SC),:]=acc2[f,t]+r3[f,t,0]+r3[f,t,1]+r3[f,t,2]
            s=g_ref.at[core,pl.ds(me,SC),:]
            for o in OS: go(s,s,K(f,3,t,o),peer(A2[t],o)[0])
    def st5(f):
        for t in range(3):
            for o in OS:
                s=g_ref.at[core,pl.ds(al8(mine(f,t)+src(A2[t],o)*SC),SC),:]
                rc(s,s,K(f,3,t,o),partner).wait_recv()
            s=g_ref.at[core,pl.ds(al8(mine(f,t)),CH),:]
            for o in OS: rc(s,s,K(f,4,t,o),peer(A1[t],o)[0]).start()
    def c6(f,t,k):
        s=g_ref.at[k,pl.ds(f*PH+t*TH,TH),:]
        return rc(s,s,136+f*3+t,partner)
    def st6(f,keep=True):
        for t in range(3):
            for o in OS:
                s=g_ref.at[core,pl.ds(al8(f*PH+t*TH+src(A1[t],o)*CH),CH),:]
                rc(s,s,K(f,4,t,o),partner).wait_recv()
            c6(f,t,core).start()
    def fin(f):
        for t in range(3): c6(f,t,1-core).wait_recv()
    gram(1,[0,1])
    st1(0)
    gram(1,[2,3,4,5,6,7])
    st1(1); st2(0); st1(2)
    def comm_rest():
        st3(0); st2(1)
        st4(0); st3(1); st2(2)
        st5(0); st4(1); st3(2)
        st6(0); st5(1); st4(2)
        fin(0); st6(1); st5(2)
    def hook(kk):
        @pl.when(kk==1)
        def _():
            fin(1); st6(2)
        @pl.when(kk==3)
        def _():
            fin(2)
    def blk(p):
        return jnp.concatenate([g_ref[0,pl.ds(p*64,64),:],g_ref[1,pl.ds(p*64,64),:]],axis=0)
    def splitx(x):
        xh,xl=split(x)
        return jnp.concatenate([xh,xl],axis=0)
    def mul3(ph,plo,r):
        t=dnt(ph,r)
        return t[:,:LB]+t[:,LB:]+dnt(plo,r[:LB])
    def mk(rlo,K):
      def body(kk,_):
        if rlo<512: hook(kk)
        c0=pl.multiple_of(kk*LB,LB)
        off=kk*8-lax.shift_right_logical(kk*(kk-1),1)
        W=[d_ref[8*g:8*g+8,:] for g in range(16)]
        X=leaf(W)
        cp=pl.multiple_of(jnp.maximum(kk-1,0)*LB,LB)
        xs=xs_ref[...]
        ph,plo=split(c_ref[rlo:T,:])
        l=mul3(ph,plo,xs)
        h,lw=split(l)
        hi_ref[rlo:T,pl.ds(cp,LB)]=h; lo_ref[rlo:T,pl.ds(cp,LB)]=lw
        q_ref[:,pl.ds(cp,LB)]=l[NB-rlo:]
        rh=jnp.concatenate([hi_ref[pl.ds(c0,LB),0:K],lo_ref[pl.ds(c0,LB),0:K]],axis=0)
        u=mul3(hi_ref[rlo:T,0:K],lo_ref[rlo:T,0:K],rh)
        for r0 in range(rlo,NB,LB):
            c_ref[r0:r0+LB,:]=blk(off+r0//LB-kk)-u[r0-rlo:r0-rlo+LB]
        c_ref[NB:T,:]=a_ref[:,pl.ds(c0,LB)]-u[NB-rlo:]
        kn=jnp.minimum(kk+1,7); n0=pl.multiple_of(kn*LB,LB)
        nh=hi_ref[pl.ds(n0,LB),0:K]; nl=lo_ref[pl.ds(n0,LB),0:K]
        dn=blk(kn*8-lax.shift_right_logical(kn*(kn-1),1))-mul3(nh,nl,jnp.concatenate([nh,nl],axis=0))
        xn=splitx(jnp.concatenate(X,axis=0))
        xs_ref[...]=xn
        ph,plo=split(c_ref[pl.ds(n0,LB),:])
        l=mul3(ph,plo,xn)
        h,lw=split(l)
        d_ref[...]=dn-mul3(h,lw,jnp.concatenate([h,lw],axis=0))
        return 0
      return body
    comm_rest()
    d_ref[...]=blk(0)
    lax.fori_loop(0,2,mk(0,256),0)
    lax.fori_loop(2,4,mk(256,512),0)
    lax.fori_loop(4,6,mk(512,768),0)
    lax.fori_loop(6,8,mk(768,1024),0)
    ph,plo=split(c_ref[NB:T,:])
    q_ref[:,7*LB:]=mul3(ph,plo,xs_ref[...])

    for c in sends: c.wait_send()
    for f in range(3):
        for t in range(3):
            c6(f,t,core).wait_send()
            s=g_ref.at[core,pl.ds(al8(mine(f,t)),CH),:]
            for o in OS: rc(s,s,K(f,4,t,o),partner).wait_send()

def solution(mesh):
    VM=pltpu.VMEM
    V=pl.BlockSpec(memory_space=VM)
    def body(a):
        return pl.pallas_call(kernel, out_shape=jax.ShapeDtypeStruct((R,NB),F),
            in_specs=[pl.BlockSpec(memory_space=pltpu.HBM)], out_specs=V, name="ortho",
            scratch_shapes=[VM((R,NB),F),VM((2,ROWS,LB),F),VM((R,NB),F),VM((2,R,NB),BF),VM((2,R,NB),BF),VM((2,NB,R),BF),VM((2,NB,R),BF),
                VM((ROWS,LB),F),VM((3,3,3,CH,LB),F),VM((3,3,CH,LB),F),VM((3,3,3,SC,LB),F),VM((3,3,SC,LB),F),VM((3,3,3,SC,LB),F),
                VM((T,NB),BF),VM((T,NB),BF),VM((T,LB),F),VM((2*LB,LB),BF),VM((LB,LB),F),
                pltpu.SemaphoreType.DMA((145,)),pltpu.SemaphoreType.DMA((145,)),pltpu.SemaphoreType.DMA],
            compiler_params=pltpu.CompilerParams(collective_id=0,has_side_effects=True,vmem_limit_bytes=48*1024*1024))(a)
    spec = P_(("row", "col"), None)
    return jax.shard_map(body, mesh=mesh, in_specs=spec, out_specs=spec, check_vma=False)
```

```python
import jax
import jax.numpy as jnp
from jax import lax
from jax.experimental import pallas as pl
from jax.experimental.pallas import tpu as pltpu
from jax.sharding import PartitionSpec as P_

def bl(x, c):
    return jnp.take_along_axis(x, jnp.full((8,128), c, jnp.int32), axis=1, mode='promise_in_bounds')
def bs(x, k):
    return jnp.broadcast_to(x[k:k+1, :], (8,128))

def leaf(W, near=4, full=2):
    BF=jnp.bfloat16; F=jnp.float32
    sub = lax.broadcasted_iota(jnp.int32, (8,128), 0)
    lane = lax.broadcasted_iota(jnp.int32, (8,128), 1)
    W = list(W)
    out = [None]*16
    rv = jnp.zeros((8,128), F)
    for G in range(8):
        g0, g1 = 2*G, 2*G+1
        nf = list(range(2*G+2, min(2*G+2+full,16)))
        nh = list(range(2*G+2+full, min(2*G+2+near,16)))
        base = 16*G
        far = 2*G+2+near < 16
        C = {}
        for k in range(16):
            for h in ([g0] if k < 8 else []) + [g1] + nf + (nh if k < 8 else []):
                C[h, k] = bl(W[h], base+k)
        U = {}
        dn = None
        for k in range(16):
            if k == 8:
                for h in nh:
                    for kk in range(8, 16): C[h, kk] = bl(W[h], base+kk)
            own, i = (g0, k) if k < 8 else (g1, k-8)
            act = ([g0] if k < 8 else []) + [g1] + nf + nh
            d = bs(C[own, k], i) if dn is None else dn
            r = 1.0/d
            rs = lax.rsqrt(d)
            if k < 15:
                o2, i2 = (g0, k+1) if k+1 < 8 else (g1, k-7)
                cc = bs(C[o2, k], i2)
                dn = bs(C[o2, k+1], i2) - (cc*cc)*r
            m = {h: C[h, k]*r for h in act}
            for j in range(k+1, 16):
                s = bs(C[g0, k], j) if j < 8 else bs(C[g1, k], j-8)
                for h in ([g0] if j < 8 else []) + [g1] + nf + (nh if (j < 8 or k >= 8) else []):
                    C[h, j] = C[h, j] - m[h]*s
            wr = bs(W[own], i)
            hot = lane == base+k
            wr2 = jnp.where(hot, wr+wr, wr)
            for h in act:
                if h == own and i == 7: continue
                W[h] = W[h] - m[h]*wr2
            fx = wr*rs
            out[own] = fx if i == 0 else jnp.where(sub == i, fx, out[own])
            rv = jnp.where(hot, r, rv)
        if far:
            u = jnp.concatenate([out[g0], out[g1]], axis=0)
            cl = lax.broadcasted_iota(jnp.int32, (16,128), 1)
            rw = lax.broadcasted_iota(jnp.int32, (16,128), 0)
            ub = jnp.where((cl <= base+rw) | (cl >= base+16), u, 0.0)
            h = ub.astype(BF); l = (ub - h.astype(F)).astype(BF)
            ur = jnp.where(cl >= base+16, u, 0.0)
            hr = ur.astype(BF); lr = (ur - hr.astype(F)).astype(BF)
            a = jnp.concatenate([hr, hr, lr], axis=0)
            b = jnp.concatenate([h, l, h], axis=0)
            upd = lax.dot_general(a, b, (((0,),(0,)),((),())), preferred_element_type=F)
            keep = (lane < base) | (lane >= base+16)
            for q in range(2*G+2+near, 16):
                W[q] = jnp.where(keep, W[q], 0.0) - upd[8*q:8*q+8, :]
    res = []
    for g in range(16):
        res.append(jnp.where(lane <= sub + 8*g, out[g]*rv, 0.0))
    return res

NB=1024; R=160; LB=128; T=NB+R; NG=20480
F=jnp.float32; BF=jnp.bfloat16
NT=(((1,),(1,)),((),())); NN=(((1,),(0,)),((),()))
MESH=pl.DeviceIdType.MESH
def dnt(a,b): return lax.dot_general(a,b,NT,preferred_element_type=F)
def dnn(a,b): return lax.dot_general(a,b,NN,preferred_element_type=F)
def split(x):
    hi=x.astype(BF); lo=(x-hi.astype(F)).astype(BF)
    return hi,lo
ROWS=36*64; PH=ROWS//3; TH=PH//3; CH=TH//4; SC=CH//4
OFF=[j*8-j*(j-1)//2 for j in range(9)]

def kernel(x_ref, q_ref, a_ref, g_ref, b_ref, ah, al, th, tl, p_ref, r1, acc1, r2, acc2, r3,
           hi_ref, lo_ref, c_ref, xs_ref, d_ref, ssem, rsem, lsem):
    row=lax.axis_index("row"); col=lax.axis_index("col")
    core=lax.rem(row,2); crd=[lax.rem(col,4), lax.div(row,2), lax.div(col,4)]
    def dev(c,k): return (c[1]*2+k, c[2]*4+c[0])
    def peer(ax,o):
        c=list(crd); c[ax]=lax.rem(crd[ax]+o,4); return dev(c,core), c[ax]
    def src(ax,o): return lax.rem(crd[ax]+(4-o),4)
    partner=dev(crd,1-core)
    bar=pltpu.get_barrier_semaphore()
    pl.semaphore_signal(bar,inc=1,device_id=partner,device_id_type=MESH)
    for ax in range(3):
        for o in (1,2,3):
            pl.semaphore_signal(bar,inc=1,device_id=peer(ax,o)[0],device_id_type=MESH)
    sends=[]
    def rc(s,d,k,to):
        return pltpu.make_async_remote_copy(src_ref=s,dst_ref=d,send_sem=ssem.at[k],recv_sem=rsem.at[k],device_id=to,device_id_type=MESH)
    def go(s,d,k,to):
        c=rc(s,d,k,to); c.start(); sends.append(c); return c
    def prep(x,n):
        h,l=split(x)
        ah[n]=h; al[n]=l
        for i in range(8):
            th[n,i*LB:(i+1)*LB,:]=h[:,i*LB:(i+1)*LB].T
            tl[n,i*LB:(i+1)*LB,:]=l[:,i*LB:(i+1)*LB].T
    h64=pl.multiple_of(core*64,64)
    def gram(n,js):
        lh=jnp.concatenate([th[n,pl.ds(i*LB+h64,64),:] for i in range(js[0],8)],axis=0)
        ll=jnp.concatenate([tl[n,pl.ds(i*LB+h64,64),:] for i in range(js[0],8)],axis=0)
        for j in js:
            bh=ah[n,:,j*LB:(j+1)*LB]; bl_=al[n,:,j*LB:(j+1)*LB]
            z=64*(j-js[0])
            t=dnn(lh[z:],jnp.concatenate([bh,bl_],axis=1))
            u=t[:,:LB]+t[:,LB:]+dnn(ll[z:],bh)
            s=slice(OFF[j]*64,OFF[j+1]*64)
            if n==0: p_ref[s,:]=u
            else: p_ref[s,:]=(p_ref[s,:]+u)*(1.0/NG)
    ld=pltpu.make_async_copy(x_ref,a_ref,lsem); ld.start()
    hi_ref[...]=jnp.zeros_like(hi_ref); lo_ref[...]=jnp.zeros_like(lo_ref)
    c_ref[...]=jnp.zeros_like(c_ref); xs_ref[...]=jnp.zeros_like(xs_ref)
    ld.wait()
    prep(a_ref[...],0)
    pl.semaphore_wait(bar,10)
    ca=go(a_ref,b_ref,0,partner)
    gram(0,list(range(8)))
    ca.wait_recv()
    prep(b_ref[...],1)
    al8=lambda v: pl.multiple_of(v,8)
    def K(f,st,t,o): return 1+(f*5+st)*9+t*3+(o-1)
    A1=[0,1,2]; A2=[1,2,0]; A3=[2,0,1]
    OS=(2,1,3); C={}
    def st1(f):
        for t in range(3):
            for o in OS:
                d,ci=peer(A1[t],o)
                C[f,1,t,o]=go(p_ref.at[pl.ds(al8(f*PH+t*TH+ci*CH),CH),:], r1.at[f,t,o-1], K(f,0,t,o), d)
    def st2(f):
        for t in range(3):
            for o in OS: C[f,1,t,o].wait_recv()
            acc1[f,t]=p_ref[pl.ds(al8(f*PH+t*TH+crd[A1[t]]*CH),CH),:]+r1[f,t,0]+r1[f,t,1]+r1[f,t,2]
            for o in OS:
                d,ci=peer(A2[t],o)
                C[f,2,t,o]=go(acc1.at[f,t,pl.ds(al8(ci*SC),SC),:], r2.at[f,t,o-1], K(f,1,t,o), d)
    def st3(f):
        for t in range(3):
            for o in OS: C[f,2,t,o].wait_recv()
            acc2[f,t]=acc1[f,t,pl.ds(al8(crd[A2[t]]*SC),SC),:]+r2[f,t,0]+r2[f,t,1]+r2[f,t,2]
            for o in OS:
                d,ci=peer(A3[t],o)
                C[f,3,t,o]=go(acc2.at[f,t], r3.at[f,t,o-1], K(f,2,t,o), d)
    def mine(f,t): return f*PH+t*TH+crd[A1[t]]*CH
    def st4(f):
        for t in range(3):
            for o in OS: C[f,3,t,o].wait_recv()
            me=al8(mine(f,t)+crd[A2[t]]*SC)
            g_ref[core,pl.ds(me,SC),:]=acc2[f,t]+r3[f,t,0]+r3[f,t,1]+r3[f,t,2]
            s=g_ref.at[core,pl.ds(me,SC),:]
            for o in OS: go(s,s,K(f,3,t,o),peer(A2[t],o)[0])
    def st5(f):
        for t in range(3):
            for o in OS:
                s=g_ref.at[core,pl.ds(al8(mine(f,t)+src(A2[t],o)*SC),SC),:]
                rc(s,s,K(f,3,t,o),partner).wait_recv()
            s=g_ref.at[core,pl.ds(al8(mine(f,t)),CH),:]
            for o in OS: rc(s,s,K(f,4,t,o),peer(A1[t],o)[0]).start()
    def c6(f,t,k):
        s=g_ref.at[k,pl.ds(f*PH+t*TH,TH),:]
        return rc(s,s,136+f*3+t,partner)
    def st6(f,keep=True):
        for t in range(3):
            for o in OS:
                s=g_ref.at[core,pl.ds(al8(f*PH+t*TH+src(A1[t],o)*CH),CH),:]
                rc(s,s,K(f,4,t,o),partner).wait_recv()
            c6(f,t,core).start()
    def fin(f):
        for t in range(3): c6(f,t,1-core).wait_recv()
    gram(1,[0,1])
    st1(0)
    gram(1,[2,3,4,5,6,7])
    st1(1); st2(0); st1(2)
    def comm_rest():
        st3(0); st2(1)
        st4(0); st3(1); st2(2)
        st5(0); st4(1); st3(2)
        st6(0); st5(1); st4(2)
        fin(0)
    def hook(kk):
        @pl.when(kk==1)
        def _():
            st6(1); st5(2); fin(1)
        @pl.when(kk==2)
        def _():
            st6(2)
        @pl.when(kk==3)
        def _():
            fin(2)
    def blk(p):
        return jnp.concatenate([g_ref[0,pl.ds(p*64,64),:],g_ref[1,pl.ds(p*64,64),:]],axis=0)
    def splitx(x):
        xh,xl=split(x)
        return jnp.concatenate([xh,xl],axis=0)
    def mul3(ph,plo,r):
        t=dnt(ph,r)
        return t[:,:LB]+t[:,LB:]+dnt(plo,r[:LB])
    def mk(rlo,K):
      def body(kk,_):
        if rlo<512: hook(kk)
        c0=pl.multiple_of(kk*LB,LB)
        off=kk*8-lax.shift_right_logical(kk*(kk-1),1)
        W=[d_ref[8*g:8*g+8,:] for g in range(16)]
        X=leaf(W)
        cp=pl.multiple_of(jnp.maximum(kk-1,0)*LB,LB)
        xs=xs_ref[...]
        ph,plo=split(c_ref[rlo:T,:])
        l=mul3(ph,plo,xs)
        h,lw=split(l)
        hi_ref[rlo:T,pl.ds(cp,LB)]=h; lo_ref[rlo:T,pl.ds(cp,LB)]=lw
        q_ref[:,pl.ds(cp,LB)]=l[NB-rlo:]
        rh=jnp.concatenate([hi_ref[pl.ds(c0,LB),0:K],lo_ref[pl.ds(c0,LB),0:K]],axis=0)
        u=mul3(hi_ref[rlo:T,0:K],lo_ref[rlo:T,0:K],rh)
        for r0 in range(rlo,NB,LB):
            c_ref[r0:r0+LB,:]=blk(off+r0//LB-kk)-u[r0-rlo:r0-rlo+LB]
        c_ref[NB:T,:]=a_ref[:,pl.ds(c0,LB)]-u[NB-rlo:]
        kn=jnp.minimum(kk+1,7); n0=pl.multiple_of(kn*LB,LB)
        nh=hi_ref[pl.ds(n0,LB),0:K]; nl=lo_ref[pl.ds(n0,LB),0:K]
        dn=blk(kn*8-lax.shift_right_logical(kn*(kn-1),1))-mul3(nh,nl,jnp.concatenate([nh,nl],axis=0))
        xn=splitx(jnp.concatenate(X,axis=0))
        xs_ref[...]=xn
        ph,plo=split(c_ref[pl.ds(n0,LB),:])
        l=mul3(ph,plo,xn)
        h,lw=split(l)
        d_ref[...]=dn-mul3(h,lw,jnp.concatenate([h,lw],axis=0))
        return 0
      return body
    comm_rest()
    d_ref[...]=blk(0)
    lax.fori_loop(0,2,mk(0,256),0)
    lax.fori_loop(2,4,mk(256,512),0)
    lax.fori_loop(4,6,mk(512,768),0)
    lax.fori_loop(6,8,mk(768,1024),0)
    ph,plo=split(c_ref[NB:T,:])
    q_ref[:,7*LB:]=mul3(ph,plo,xs_ref[...])

    for c in sends: c.wait_send()
    for f in range(3):
        for t in range(3):
            c6(f,t,core).wait_send()
            s=g_ref.at[core,pl.ds(al8(mine(f,t)),CH),:]
            for o in OS: rc(s,s,K(f,4,t,o),partner).wait_send()

def solution(mesh):
    VM=pltpu.VMEM
    V=pl.BlockSpec(memory_space=VM)
    def body(a):
        return pl.pallas_call(kernel, out_shape=jax.ShapeDtypeStruct((R,NB),F),
            in_specs=[pl.BlockSpec(memory_space=pltpu.HBM)], out_specs=V, name="ortho",
            scratch_shapes=[VM((R,NB),F),VM((2,ROWS,LB),F),VM((R,NB),F),VM((2,R,NB),BF),VM((2,R,NB),BF),VM((2,NB,R),BF),VM((2,NB,R),BF),
                VM((ROWS,LB),F),VM((3,3,3,CH,LB),F),VM((3,3,CH,LB),F),VM((3,3,3,SC,LB),F),VM((3,3,SC,LB),F),VM((3,3,3,SC,LB),F),
                VM((T,NB),BF),VM((T,NB),BF),VM((T,LB),F),VM((2*LB,LB),BF),VM((LB,LB),F),
                pltpu.SemaphoreType.DMA((145,)),pltpu.SemaphoreType.DMA((145,)),pltpu.SemaphoreType.DMA],
            compiler_params=pltpu.CompilerParams(collective_id=0,has_side_effects=True,vmem_limit_bytes=48*1024*1024))(a)
    spec = P_(("row", "col"), None)
    return jax.shard_map(body, mesh=mesh, in_specs=spec, out_specs=spec, check_vma=False)
```
